256 devices in a mesh: seq: 128 (over x, y, z_lo, core), fsdp: 2 (over z_hi).
Axes of the slice: x: 4, y: 4, z: 8 (z_hi: 2, z_lo: 4; z = z_hi * 4 + z_lo), core: 2. Of those that a mesh axis runs over, the one named last changes fastest.
Arguments:
- queries: bfloat16 [65536, 2048], P(('seq', 'fsdp')), may hold values from -150 to 150
- key_rotated_rows: bfloat16 [65536, 1024], P(('seq', 'fsdp')), may hold values from -5 to 5
- values: bfloat16 [65536, 1024], P(('seq', 'fsdp')), may hold values from -6 to 6
- out_weight: bfloat16 [2048, 5376], P('seq', 'fsdp'), may hold values from -0.125 to 0.125
- residual: bfloat16 [65536, 5376], P(('seq', 'fsdp')), may hold values from -6 to 6
- norm_gain: float32 [5376], replicated, may hold values from 0.25 to 1.75
- doc_lengths: int32 [64], replicated, may hold values from 1 to 2048, 65536 in all
Outputs:
- output: bfloat16 [65536, 5376], P(('seq', 'fsdp'))
The draws below stay inside these ranges and needn't reach their ends.
All inputs are finite; a program needn't handle non-finite values.
Results may differ from the reference program's by a relative error of at most 0.007.
Values may be sent and summed in bfloat16 or wider, within the bound.
A program may use at most 128 MiB of HBM per device.

```python
import math
import jax
import jax.numpy as jnp
import numpy as np
from jax import lax

D = 5376
QUERY_HEADS = 16
KEY_VALUE_HEADS = 8
HEAD_SIZE = 128
WINDOW_TOKENS = 1024
QSCALE = 168
TOKENS_PER_SHARD = 256
CONTEXT_TOKENS = 65536
DOCS = 64


def draw_pair(key):
    base = jax.random.fold_in(key, 4242)
    first_segment, part_b = jax.random.split(base, 2)
    key_rotated_rows = jnp.clip(jax.random.normal(first_segment, (CONTEXT_TOKENS, KEY_VALUE_HEADS * HEAD_SIZE), jnp.float32), -4.5, 4.5)
    queries = jnp.clip(jax.random.normal(part_b, (CONTEXT_TOKENS, QUERY_HEADS * HEAD_SIZE), jnp.float32), -4.0, 4.0)
    return (queries, key_rotated_rows)


def draw_queries(key, part):
    return draw_pair(key)[0].astype(jnp.bfloat16)


def draw_key_rotated_rows(key, part):
    return draw_pair(key)[1].astype(jnp.bfloat16)


def block_scale(stream_key, shape, shards, low, high):
    level, own = 1.0, jax.random.fold_in(stream_key, 6)
    for position, blocks in shards:
        heights = jnp.exp(jax.random.uniform(jax.random.fold_in(own, position), (blocks,), jnp.float32, low / len(shards), high / len(shards)))
        level = level * jnp.repeat(heights, shape[position] // blocks).reshape([-1 if axis == position else 1 for axis in range(len(shape))])
    return level


def split_up(number_of, total, reach, lean):
    portions = [(1 << 20) // math.isqrt(rank ** lean) + 1 for rank in range(2, number_of + 1)]
    rest, holding = total - reach - (number_of - 1), [1] * (number_of - 1)
    while rest > 0:
        free = [i for i in range(number_of - 1) if holding[i] < reach]
        mass, remaining = sum([portions[i] for i in free]), rest
        for i in free:
            addition = min(reach - holding[i], max(1, remaining * portions[i] // mass), rest)
            holding[i] = holding[i] + addition
            rest = rest - addition
    return np.array([reach] + holding)


def uneven_parts(key, number_of, total, reach, slope):
    if number_of == 2:
        one = jax.random.randint(key, (), max(1, total - reach), min(reach, total - 1) + 1)
        return jnp.stack([one, total - one])
    sizes = jnp.asarray(split_up(number_of, total, reach, slope), jnp.int32)
    pairs = (number_of - 1) // 2
    donor, sink = sizes[1:1 + 2 * pairs:2], sizes[2:2 + 2 * pairs:2]
    slack = jnp.minimum(donor - 1, reach - sink)
    shifted = jax.random.randint(jax.random.fold_in(key, 1), (pairs,), 0, 1 << 20) % (slack + 1)
    sizes = sizes.at[1:1 + 2 * pairs:2].set(donor - shifted).at[2:2 + 2 * pairs:2].set(sink + shifted)
    return sizes[jax.random.permutation(jax.random.fold_in(key, 2), number_of)]


def centred(own_key, dims, deviation, limit, shards=(), kind=jnp.bfloat16):
    array = deviation * jax.random.normal(own_key, dims, jnp.float32)
    if shards:
        array = array * block_scale(own_key, dims, shards, -0.22, 0.18)
    return jnp.clip(array, -limit, limit).astype(kind)


def setup_inputs(seed: int = 0) -> dict:
    keys = jax.random.split(jax.random.key(seed), 8)
    return {
        "queries": draw_queries(jax.random.fold_in(keys[7], 71), 0),
        "key_rotated_rows": draw_key_rotated_rows(jax.random.fold_in(keys[7], 71), 0),
        "values": centred(keys[2], (CONTEXT_TOKENS, KEY_VALUE_HEADS * HEAD_SIZE), 1.0, 6.0, ((0, 256),)),
        "out_weight": centred(keys[3], (QUERY_HEADS * HEAD_SIZE, D), (QUERY_HEADS * HEAD_SIZE) ** -0.5, 0.125, ((0, 128), (1, 2))),
        "residual": centred(keys[4], (CONTEXT_TOKENS, D), 1.0, 6.0, ((0, 256),)),
        "norm_gain": jnp.clip(1.0 + 0.15 * jax.random.normal(keys[5], (D,), jnp.float32), 0.25, 1.75),
        "doc_lengths": uneven_parts(keys[6], DOCS, CONTEXT_TOKENS, 8 * TOKENS_PER_SHARD, 2).astype(jnp.int32),
    }


def doc_index(positions, starts):
    return lax.optimization_barrier(jnp.sum((starts[None, :] <= positions[:, None]).astype(jnp.int32), axis=1)) - 1

def reference(queries, key_rotated_rows, values, out_weight, residual, norm_gain, doc_lengths):
    queries_per_group = QUERY_HEADS // KEY_VALUE_HEADS
    scaling = QSCALE ** (-0.5)
    starts = jnp.cumsum(doc_lengths) - doc_lengths
    key_padded_rows = jnp.concatenate([jnp.zeros((WINDOW_TOKENS, KEY_VALUE_HEADS * HEAD_SIZE), key_rotated_rows.dtype), key_rotated_rows], axis=0)
    value_padded_rows = jnp.concatenate([jnp.zeros((WINDOW_TOKENS, KEY_VALUE_HEADS * HEAD_SIZE), values.dtype), values], axis=0)

    def block(block_index):
        token_offset = (block_index * TOKENS_PER_SHARD).astype(jnp.int32)
        query_block_tile = lax.dynamic_slice_in_dim(queries, token_offset, TOKENS_PER_SHARD, 0).reshape(TOKENS_PER_SHARD, KEY_VALUE_HEADS, queries_per_group, HEAD_SIZE).astype(jnp.float32)
        key_block_tile = lax.dynamic_slice_in_dim(key_padded_rows, token_offset, WINDOW_TOKENS + TOKENS_PER_SHARD, 0).reshape(WINDOW_TOKENS + TOKENS_PER_SHARD, KEY_VALUE_HEADS, HEAD_SIZE).astype(jnp.float32)
        value_block_tile = lax.dynamic_slice_in_dim(value_padded_rows, token_offset, WINDOW_TOKENS + TOKENS_PER_SHARD, 0).reshape(WINDOW_TOKENS + TOKENS_PER_SHARD, KEY_VALUE_HEADS, HEAD_SIZE).astype(jnp.float32)
        q_pos = token_offset + jnp.arange(TOKENS_PER_SHARD, dtype=jnp.int32)
        k_pos = token_offset - WINDOW_TOKENS + jnp.arange(WINDOW_TOKENS + TOKENS_PER_SHARD, dtype=jnp.int32)
        lag = q_pos[:, None] - k_pos[None, :]
        allowed = (doc_index(q_pos, starts)[:, None] == doc_index(k_pos, starts)[None, :]) & (lag >= 0) & (lag < WINDOW_TOKENS) & (k_pos[None, :] >= 0)
        scores = jnp.einsum('qhgd,khd->hgqk', query_block_tile, key_block_tile) * scaling
        scores = jnp.where(allowed[None, None], scores, -jnp.inf)
        peak = lax.optimization_barrier(jnp.max(scores, axis=-1, keepdims=True))
        expon = jnp.exp(scores - peak)
        probs = (expon / lax.optimization_barrier(jnp.sum(expon, axis=-1, keepdims=True))).astype(jnp.bfloat16)
        mixed = jnp.einsum('hgqk,khd->qhgd', probs.astype(jnp.float32), value_block_tile)
        return mixed.reshape(TOKENS_PER_SHARD, QUERY_HEADS * HEAD_SIZE).astype(jnp.bfloat16)
    attended = lax.map(block, jnp.arange(CONTEXT_TOKENS // TOKENS_PER_SHARD, dtype=jnp.int32)).reshape(CONTEXT_TOKENS, QUERY_HEADS * HEAD_SIZE)
    projected = jnp.dot(attended, out_weight, preferred_element_type=jnp.float32)
    meansq = lax.optimization_barrier(jnp.mean(projected * projected, axis=-1, keepdims=True))
    output = residual.astype(jnp.float32) + norm_gain.astype(jnp.float32) * projected * lax.rsqrt(meansq + 1e-06)
    return output.astype(jnp.bfloat16)
```

```python
import functools
import math

import jax
import jax.numpy as jnp
from jax import lax
from jax.experimental import pallas as pl
from jax.experimental.pallas import tpu as pltpu
from jax.sharding import PartitionSpec as P

QUERY_HEADS = 16
KEY_VALUE_HEADS = 8
HEAD_SIZE = 128
WINDOW = 1024
QSCALE = 168
ROWS = 256
D = 5376
HALF = D // 2
CHUNKS = 4
CHUNK_COLS = KEY_VALUE_HEADS * HEAD_SIZE // CHUNKS
STAGES = 8
TICKS = STAGES + 4
MESH = pl.DeviceIdType.MESH


def coordinates():
    s = lax.axis_index("seq")
    zh = lax.axis_index("fsdp")
    core = s % 2
    zl = (s // 2) % 4
    y = (s // 8) % 4
    x = s // 32
    return s, zh, core, zl, y, x


def comm_kernel(
    k_ref, v_ref, w_ref, kb, vb, wb,
    local_sem, zs, zr, fs, fr, ss, sr, ds, dr, kvs, kvr,
):
    s, zh, core, zl, y, x = coordinates()
    z = zh * 4 + zl
    f = x + core * (y - x)
    g = y + core * (x - y)
    f_stride = 32 - 24 * core
    g_stride = 8 + 24 * core

    def device(seq, fsdp):
        return {"seq": seq, "fsdp": fsdp}

    def at_z(step):
        to = (z + step + 8) % 8
        return device(s + 2 * (to % 4 - zl), to // 4)

    def at_f(step):
        return device(s + f_stride * ((f + step + 4) % 4 - f), zh)

    def at_g(step):
        return device(s + g_stride * ((g + step + 4) % 4 - g), zh)

    def at_pair(step, fsdp, to_core):
        return device((s - core + 2 * step + 128) % 128 + to_core, fsdp)

    partner = device(s + 1 - 2 * core, zh)

    barrier = pltpu.get_barrier_semaphore()
    known = [at_z(1), at_z(-1), at_f(1), at_f(-1), at_g(1), at_g(-1), partner]
    for step in (-1, 1):
        for fsdp in (0, 1):
            for to_core in (0, 1):
                known.append(at_pair(step, fsdp, to_core))
    for to_core in (0, 1):
        known.append(at_pair(0, 1 - zh, to_core))
    for who in known:
        pl.semaphore_signal(barrier, inc=1, device_id=who, device_id_type=MESH)
    own = pltpu.make_async_copy(w_ref, wb.at[core, z, g, f], local_sem)
    own.start()
    pl.semaphore_wait(barrier, len(known))

    def remote(src, dst, send, recv, who):
        return pltpu.make_async_remote_copy(
            src_ref=src, dst_ref=dst, send_sem=send, recv_sem=recv, device_id=who, device_id_type=MESH
        )

    def cols(chunk):
        return pl.ds(pl.multiple_of(chunk * CHUNK_COLS, CHUNK_COLS), CHUNK_COLS)

    def kv_pair(src, slot, chunk, send_row, who):
        out = []
        for n, (mine, buf) in enumerate(((k_ref, kb), (v_ref, vb))):
            source = mine.at[:, cols(chunk)] if src is None else buf.at[src, :, cols(chunk)]
            out.append(
                remote(source, buf.at[slot, :, cols(chunk)], kvs.at[send_row, chunk, n], kvr.at[slot, chunk, n], who)
            )
        return out

    def start(copies):
        for copy in copies:
            copy.start()

    def arrived(slot, chunk):
        for copy in kv_pair(slot, slot, chunk, 0, partner):
            copy.wait_recv()

    is_a = zh == 0
    first = core == 0
    has_opposite = jnp.logical_not(jnp.logical_and(is_a, first))
    has_three = jnp.logical_not(jnp.logical_and(zh == 1, core == 1))
    opposite_core = core * zh
    three_core = jnp.where(first, 1, 0)
    three_step = jnp.where(first, -1, 0)

    def route0(chunk):
        return kv_pair(None, 0, chunk, 0, at_pair(1, zh, core))

    def route1(chunk):
        return kv_pair(None, 1, chunk, 1, at_pair(1, 1 - zh, opposite_core))

    def route2_own(chunk):
        return kv_pair(None, 2, chunk, 2, partner)

    def route2_relay(chunk):
        return kv_pair(0, 2, chunk, 2, partner)

    def route3(chunk):
        return kv_pair(1, 3, chunk, 3, at_pair(three_step, zh, three_core))

    def route4_a(chunk):
        return kv_pair(0, 3, chunk, 4, at_pair(-1, 1, 0))

    def route4_b(chunk):
        return kv_pair(3, 1, chunk, 4, partner)

    def kv_begin(chunk, _):
        start(route0(chunk))

        @pl.when(has_opposite)
        def _():
            start(route1(chunk))

        @pl.when(first)
        def _():
            start(route2_own(chunk))

        return 0

    def kv_relay_near(chunk):
        arrived(0, chunk)

        @pl.when(core == 1)
        def _():
            start(route2_relay(chunk))

        @pl.when(jnp.logical_and(is_a, first))
        def _():
            start(route4_a(chunk))

    def kv_relay_far(chunk):
        @pl.when(has_three)
        def _():
            arrived(1, chunk)
            start(route3(chunk))

    def kv_relay_last(chunk):
        arrived(3, chunk)

        @pl.when(jnp.logical_and(zh == 1, first))
        def _():
            start(route4_b(chunk))

    def kv_finish(chunk):
        arrived(2, chunk)

        @pl.when(jnp.logical_not(has_three))
        def _():
            arrived(1, chunk)

    def piece(i):
        return (z + ((i + 1) // 2) * (1 - 2 * (i % 2)) + 8) % 8

    def z_send(src_piece, to_stage, step):
        ref = wb.at[core, src_piece, g, f]
        return remote(ref, ref, zs.at[to_stage], zr.at[to_stage], at_z(step))

    def z_recv(i):
        ref = wb.at[core, piece(i), g, f]
        return remote(ref, ref, zs.at[i], zr.at[i], partner)

    def f_copy(i, from_f, lane, step):
        ref = wb.at[core, piece(i), g, (from_f + 4) % 4]
        return remote(ref, ref, fs.at[i, lane], fr.at[i, lane], at_f(step))

    def s_copy(i, from_g, lane, step):
        ref = wb.at[core, piece(i), (from_g + 4) % 4]
        return remote(ref, ref, ss.at[i, lane], sr.at[i, lane], at_g(step))

    def s_half(i, from_g, lane, step):
        ref = wb.at[core, piece(i), (from_g + 4) % 4, pl.ds(2 * (lane - 2), 2)]
        return remote(ref, ref, ss.at[i, lane], sr.at[i, lane], at_g(step))

    def d_copy(i, from_core):
        ref = wb.at[from_core, piece(i)]
        return remote(ref, ref, ds.at[i], dr.at[i], partner)

    def forward_sign(i):
        return 1 - 2 * (i % 2)

    own.wait()
    lax.fori_loop(0, 1, kv_begin, 0)

    def tick(t, _):
        @pl.when(t == 0)
        def _():
            z_send(z, 1, 1).start()
            z_send(z, 2, -1).start()

        @pl.when(jnp.logical_and(t > 0, t < STAGES))
        def _():
            z_recv(t).wait_recv()

            @pl.when((t <= 4) | ((t == 5) & (core == 0)) | ((t == 6) & (core == 1)))
            def _():
                to_stage = jnp.minimum(t + 2, 7)
                z_send(piece(t), to_stage, 2 * (t % 2) - 1).start()

        @pl.when(t < STAGES)
        def _():
            f_copy(t, f, 0, 1).start()
            f_copy(t, f, 1, -1).start()

        @pl.when((t >= 1) & (t < STAGES + 1))
        def _():
            i = t - 1
            f_copy(i, f - 1, 0, 1).wait_recv()
            f_copy(i, f + 1, 1, -1).wait_recv()
            sign = forward_sign(i)
            f_copy(i, f - sign, 2, sign).start()

        @pl.when((t >= 2) & (t < STAGES + 2))
        def _():
            i = t - 2
            f_copy(i, f + 2, 2, 1).wait_recv()
            s_copy(i, g, 0, 1).start()
            s_copy(i, g, 1, -1).start()

        @pl.when((t >= 3) & (t < STAGES + 3))
        def _():
            i = t - 3
            s_copy(i, g - 1, 0, 1).wait_recv()
            s_copy(i, g + 1, 1, -1).wait_recv()
            s_half(i, g - 1, 2, 1).start()
            s_half(i, g + 1, 3, -1).start()

        @pl.when((t >= 4) & (t < STAGES + 4))
        def _():
            i = t - 4
            s_half(i, g + 2, 2, 1).wait_recv()
            s_half(i, g + 2, 3, -1).wait_recv()
            d_copy(i, core).start()

        @pl.when((t >= 1) & (t < CHUNKS))
        def _():
            kv_begin(t, 0)

        @pl.when((t >= 2) & (t < 2 + 2 * CHUNKS) & (t % 2 == 0))
        def _():
            chunk = (t - 2) // 2
            kv_relay_near(chunk)
            kv_relay_far(chunk)

        @pl.when((t >= 4) & (t < 4 + 2 * CHUNKS) & (t % 2 == 0))
        def _():
            chunk = (t - 4) // 2
            kv_relay_last(chunk)

        return 0

    lax.fori_loop(0, TICKS, tick, 0)

    def finish_kv(chunk, _):
        kv_finish(chunk)
        for copy in route0(chunk):
            copy.wait_send()

        @pl.when(has_opposite)
        def _():
            for copy in route1(chunk):
                copy.wait_send()

        for copy in route2_own(chunk):
            copy.wait_send()

        @pl.when(has_three)
        def _():
            for copy in route3(chunk):
                copy.wait_send()

        @pl.when(first)
        def _():
            for copy in route4_b(chunk):
                copy.wait_send()

        return 0

    lax.fori_loop(0, CHUNKS, finish_kv, 0)

    def finish_w(i, _):
        d_copy(i, 1 - core).wait_recv()
        d_copy(i, core).wait_send()
        f_copy(i, f, 0, 1).wait_send()
        f_copy(i, f, 1, 1).wait_send()
        f_copy(i, f, 2, 1).wait_send()
        s_copy(i, g, 0, 1).wait_send()
        s_copy(i, g, 1, 1).wait_send()
        s_half(i, g, 2, 1).wait_send()
        s_half(i, g, 3, 1).wait_send()

        @pl.when(i > 0)
        def _():
            z_recv(i).wait_send()

        return 0

    lax.fori_loop(0, STAGES, finish_w, 0)


def communicate(keys, values, weight):
    anyspace = pl.BlockSpec(memory_space=pl.ANY)
    dma = pltpu.SemaphoreType.DMA
    return pl.pallas_call(
        comm_kernel,
        out_shape=(
            jax.ShapeDtypeStruct((4, ROWS, 1024), jnp.bfloat16),
            jax.ShapeDtypeStruct((4, ROWS, 1024), jnp.bfloat16),
            jax.ShapeDtypeStruct((2, 8, 4, 4, 16, HALF), jnp.bfloat16),
        ),
        in_specs=[anyspace, anyspace, pl.BlockSpec(memory_space=pltpu.VMEM)],
        out_specs=(anyspace, anyspace, anyspace),
        scratch_shapes=[
            dma,
            dma((8,)), dma((8,)),
            dma((8, 3)), dma((8, 3)),
            dma((8, 4)), dma((8, 4)),
            dma((8,)), dma((8,)),
            dma((5, CHUNKS, 2)), dma((4, CHUNKS, 2)),
        ],
        compiler_params=pltpu.CompilerParams(collective_id=0, has_side_effects=True),
        name="exchange",
    )(keys, values, weight)


def low_bound(lengths, offset):
    row = lax.broadcasted_iota(jnp.int32, (64, 64), 0)
    col = lax.broadcasted_iota(jnp.int32, (64, 64), 1)
    starts_col = jnp.sum(jnp.where(col < row, lengths, 0), axis=1, keepdims=True)
    starts = jnp.sum(jnp.where(row == col, starts_col, 0), axis=0, keepdims=True)
    i = lax.broadcasted_iota(jnp.int32, (ROWS, 1), 0)
    begins = jnp.max(jnp.where(starts <= i + offset, starts, 0), axis=1, keepdims=True)
    return jnp.maximum(begins - offset + WINDOW, i + 1)


def attention_kernel(lengths_ref, q_ref, kb_ref, vb_ref, k_ref, v_ref, o_ref):
    s, zh, _, _, _, _ = coordinates()
    offset = (s * 2 + zh) * ROWS
    low = low_bound(lengths_ref[...], offset)
    factor = math.log2(math.e) * QSCALE ** (-0.5)
    keys = jnp.concatenate([kb_ref[j] for j in range(4)] + [k_ref[...]], axis=0)
    vals = jnp.concatenate([vb_ref[j] for j in range(4)] + [v_ref[...]], axis=0)
    width = WINDOW + 128
    for half in range(2):
        rows = slice(128 * half, 128 * half + 128)
        k_half = keys[128 * half : 128 * half + width]
        v_half = vals[128 * half : 128 * half + width]
        r = lax.broadcasted_iota(jnp.int32, (128, width), 1) + 128 * half
        i = lax.broadcasted_iota(jnp.int32, (128, width), 0) + 128 * half
        allowed = (r >= low[rows]) & (r <= i + WINDOW)
        for head in range(2):
            columns = slice(HEAD_SIZE * head, HEAD_SIZE * head + HEAD_SIZE)
            scores = lax.dot_general(
                q_ref[rows, columns], k_half, (((1,), (1,)), ((), ())), preferred_element_type=jnp.float32
            )
            scores = jnp.where(allowed, scores, -1e30)
            peak = jnp.max(scores, axis=1, keepdims=True)
            expon = jnp.exp2((scores - peak) * factor)
            total = jnp.sum(expon, axis=1, keepdims=True)
            mixed = jnp.dot(expon.astype(jnp.bfloat16), v_half, preferred_element_type=jnp.float32)
            o_ref[rows, columns] = (mixed / total).astype(jnp.bfloat16)


def attention(lengths, queries, kb, vb, keys, values):
    pair = 2 * HEAD_SIZE
    return pl.pallas_call(
        attention_kernel,
        grid=(KEY_VALUE_HEADS,),
        out_shape=jax.ShapeDtypeStruct((ROWS, QUERY_HEADS * HEAD_SIZE), jnp.bfloat16),
        in_specs=[
            pl.BlockSpec((1, 64), lambda h: (0, 0)),
            pl.BlockSpec((ROWS, pair), lambda h: (0, h)),
            pl.BlockSpec((4, ROWS, HEAD_SIZE), lambda h: (0, 0, h)),
            pl.BlockSpec((4, ROWS, HEAD_SIZE), lambda h: (0, 0, h)),
            pl.BlockSpec((ROWS, HEAD_SIZE), lambda h: (0, h)),
            pl.BlockSpec((ROWS, HEAD_SIZE), lambda h: (0, h)),
        ],
        out_specs=pl.BlockSpec((ROWS, pair), lambda h: (0, h)),
        name="attend",
    )(lengths, queries, kb, vb, keys, values)


TILE = 384
TILES = HALF // TILE


def project_kernel(a_ref, w_ref, res_ref, gain_ref, o_ref, acc):
    n = pl.program_id(0)
    slabs = []
    for x in range(4):
        for y in range(4):
            for zl in range(4):
                slabs.append(w_ref[0, zl, y, x])
                slabs.append(w_ref[1, zl, x, y])
    weight = jnp.concatenate(slabs, axis=0)
    acc[n] = jnp.dot(a_ref[...], weight, preferred_element_type=jnp.float32)

    @pl.when(n == 2 * TILES - 1)
    def _():
        def add(m, total):
            part = acc[m]
            return total + jnp.sum(part * part, axis=1, keepdims=True)

        square = lax.fori_loop(0, 2 * TILES, add, jnp.zeros((ROWS, 1), jnp.float32))
        level = lax.rsqrt(square * (1.0 / D) + 1e-06)
        for m in range(2 * TILES):
            columns = slice(TILE * m, TILE * m + TILE)
            normed = gain_ref[:, columns] * acc[m] * level
            o_ref[:, columns] = (res_ref[:, columns].astype(jnp.float32) + normed).astype(jnp.bfloat16)


def project(attended, wb, residual, gain):
    return pl.pallas_call(
        project_kernel,
        grid=(2 * TILES,),
        out_shape=jax.ShapeDtypeStruct((ROWS, D), jnp.bfloat16),
        in_specs=[
            pl.BlockSpec((ROWS, QUERY_HEADS * HEAD_SIZE), lambda n: (0, 0)),
            pl.BlockSpec((2, 4, 4, 4, 16, TILE), lambda n: (0, n // TILES, 0, 0, 0, n % TILES)),
            pl.BlockSpec((ROWS, D), lambda n: (0, 0)),
            pl.BlockSpec((1, D), lambda n: (0, 0)),
        ],
        out_specs=pl.BlockSpec((ROWS, D), lambda n: (0, 0)),
        scratch_shapes=[pltpu.VMEM((2 * TILES, ROWS, TILE), jnp.float32)],
        compiler_params=pltpu.CompilerParams(vmem_limit_bytes=48 * 1024 * 1024),
        name="project",
    )(attended, wb, residual, gain)


def shards(queries, key_rotated_rows, values, out_weight, residual, norm_gain, doc_lengths):
    kb, vb, wb = communicate(key_rotated_rows, values, out_weight)
    attended = attention(doc_lengths.reshape(1, 64), queries, kb, vb, key_rotated_rows, values)
    return project(attended, wb, residual, norm_gain.reshape(1, D))


def solution(mesh):
    rows = P(("seq", "fsdp"), None)
    in_specs = (rows, rows, rows, P("seq", "fsdp"), rows, P(), P())
    return jax.shard_map(shards, mesh=mesh, in_specs=in_specs, out_specs=rows, check_vma=False)
```

```python
import math

import jax
import jax.numpy as jnp
from jax import lax
from jax.experimental import pallas as pl
from jax.experimental.pallas import tpu as pltpu
from jax.sharding import PartitionSpec as P

QUERY_HEADS = 16
KEY_VALUE_HEADS = 8
HEAD_SIZE = 128
WINDOW = 1024
QSCALE = 168
ROWS = 256
D = 5376
HALF = D // 2
CHUNKS = KEY_VALUE_HEADS
STAGES = 8
TICKS = STAGES + 4
MESH = pl.DeviceIdType.MESH
FACTOR = math.log2(math.e) * QSCALE ** (-0.5)


def coordinates():
    s = lax.axis_index("seq")
    zh = lax.axis_index("fsdp")
    core = s % 2
    zl = (s // 2) % 4
    y = (s // 8) % 4
    x = s // 32
    return s, zh, core, zl, y, x


def exchange_kernel(
    lengths_ref, q_hbm, k_ref, v_ref, w_ref, o_ref, wb,
    q_ref, kb, vb, wv, low_ref,
    local_sem, lw, zs, zr, fs, fr, ss, sr, ds, dr, kvs, kvr,
):
    s, zh, core, zl, y, x = coordinates()
    z = zh * 4 + zl
    f = x + core * (y - x)
    g = y + core * (x - y)
    f_stride = 32 - 24 * core
    g_stride = 8 + 24 * core

    def device(seq, fsdp):
        return {"seq": seq, "fsdp": fsdp}

    def at_z(step):
        to = (z + step + 8) % 8
        return device(s + 2 * (to % 4 - zl), to // 4)

    def at_f(step):
        return device(s + f_stride * ((f + step + 4) % 4 - f), zh)

    def at_g(step):
        return device(s + g_stride * ((g + step + 4) % 4 - g), zh)

    def at_pair(step, fsdp, to_core):
        return device((s - core + 2 * step + 128) % 128 + to_core, fsdp)

    partner = device(s + 1 - 2 * core, zh)

    def w_cols(p):
        return pl.ds(pl.multiple_of((p // 4) * HALF, HALF), HALF)

    barrier = pltpu.get_barrier_semaphore()
    known = [at_z(1), at_z(-1), at_f(1), at_f(-1), at_g(1), at_g(-1), partner]
    for step in (-1, 1):
        for fsdp in (0, 1):
            for to_core in (0, 1):
                known.append(at_pair(step, fsdp, to_core))
    for to_core in (0, 1):
        known.append(at_pair(0, 1 - zh, to_core))
    for who in known:
        pl.semaphore_signal(barrier, inc=1, device_id=who, device_id_type=MESH)
    own_rows = pl.ds(WINDOW, ROWS)
    own = [
        pltpu.make_async_copy(w_ref, wv.at[core, zl, g, f, :, w_cols(z)], local_sem.at[0]),
        pltpu.make_async_copy(k_ref, kb.at[own_rows], local_sem.at[1]),
        pltpu.make_async_copy(v_ref, vb.at[own_rows], local_sem.at[2]),
        pltpu.make_async_copy(q_hbm, q_ref, local_sem.at[3]),
    ]
    for copy in own:
        copy.start()
    low_ref[...] = low_bound(lengths_ref[...], (s * 2 + zh) * ROWS)
    for copy in own:
        copy.wait()
    pl.semaphore_wait(barrier, len(known))

    def remote(src, dst, send, recv, who):
        return pltpu.make_async_remote_copy(
            src_ref=src, dst_ref=dst, send_sem=send, recv_sem=recv, device_id=who, device_id_type=MESH
        )

    def cols(chunk):
        return pl.ds(pl.multiple_of(chunk * HEAD_SIZE, HEAD_SIZE), HEAD_SIZE)

    def slot_rows(slot):
        return pl.ds(slot * ROWS, ROWS)

    def kv_pair(src, slot, chunk, send_row, who):
        return [
            remote(
                buf.at[slot_rows(src), cols(chunk)],
                buf.at[slot_rows(slot), cols(chunk)],
                kvs.at[send_row, chunk, n],
                kvr.at[slot, chunk, n],
                who,
            )
            for n, buf in enumerate((kb, vb))
        ]

    def start(copies):
        for copy in copies:
            copy.start()

    def arrived(slot, chunk):
        for copy in kv_pair(slot, slot, chunk, 0, partner):
            copy.wait_recv()

    def sent(send_row, chunk):
        for copy in kv_pair(4, 0, chunk, send_row, partner):
            copy.wait_send()

    first = core == 0
    a_first = jnp.logical_and(zh == 0, first)
    b_first = jnp.logical_and(zh == 1, first)
    a_second = jnp.logical_and(zh == 0, core == 1)
    b_second = jnp.logical_and(zh == 1, core == 1)
    last_of_four = zl == 3
    inner = jnp.logical_or(b_first, a_second)
    outer = jnp.logical_not(inner)
    to_opposite = jnp.logical_or(core == 1, jnp.logical_and(b_first, last_of_four))
    opposite = at_pair(1, 1 - zh, core * zh)

    def kv_begin(chunk):
        start(kv_pair(4, 0, chunk, 0, at_pair(1, zh, core)))

        @pl.when(to_opposite)
        def _():
            start(kv_pair(4, 1, chunk, 1, opposite))

        @pl.when(first)
        def _():
            start(kv_pair(4, 2, chunk, 2, partner))

    def kv_near(chunk):
        arrived(0, chunk)

        @pl.when(first)
        def _():
            start(kv_pair(0, 3, chunk, 3, at_pair(-1, 1 - zh, zh)))

        @pl.when(core == 1)
        def _():
            start(kv_pair(0, 2, chunk, 2, partner))

    def kv_far(chunk):
        @pl.when(a_second)
        def _():
            arrived(1, chunk)
            start(kv_pair(1, 3, chunk, 3, partner))

        @pl.when(b_first)
        def _():
            arrived(1, chunk)
            start(kv_pair(1, 3, chunk, 4, at_pair(-1, 1, 1)))

    def kv_last(chunk):
        @pl.when(inner)
        def _():
            arrived(3, chunk)

        @pl.when(b_first)
        def _():
            start(kv_pair(3, 1, chunk, 5, partner))

        @pl.when(jnp.logical_and(a_second, jnp.logical_not(last_of_four)))
        def _():
            start(kv_pair(3, 1, chunk, 5, at_pair(1, 0, 0)))

    def kv_done(chunk):
        arrived(2, chunk)

        @pl.when(outer)
        def _():
            arrived(1, chunk)
            arrived(3, chunk)

    def attend(head):
        pair = pl.ds(pl.multiple_of(head * 2 * HEAD_SIZE, 2 * HEAD_SIZE), 2 * HEAD_SIZE)
        width = WINDOW + 128
        for half in range(2):
            rows = slice(128 * half, 128 * half + 128)
            span = slice(128 * half, 128 * half + width)
            keys = kb[span, cols(head)]
            vals = vb[span, cols(head)]
            q = q_ref[rows, pair]
            r = lax.broadcasted_iota(jnp.int32, (128, width), 1) + 128 * half
            i = lax.broadcasted_iota(jnp.int32, (128, width), 0) + 128 * half
            allowed = (r >= low_ref[rows]) & (r <= i + WINDOW)
            outs = []
            for n in range(2):
                scores = lax.dot_general(
                    q[:, HEAD_SIZE * n : HEAD_SIZE * n + HEAD_SIZE],
                    keys,
                    (((1,), (1,)), ((), ())),
                    preferred_element_type=jnp.float32,
                )
                scores = jnp.where(allowed, scores, -1e30)
                peak = jnp.max(scores, axis=1, keepdims=True)
                expon = jnp.exp2((scores - peak) * FACTOR)
                total = jnp.sum(expon, axis=1, keepdims=True)
                mixed = jnp.dot(expon.astype(jnp.bfloat16), vals, preferred_element_type=jnp.float32)
                outs.append((mixed / total).astype(jnp.bfloat16))
            o_ref[rows, pair] = jnp.concatenate(outs, axis=1)

    def piece(i):
        return (z + ((i + 1) // 2) * (1 - 2 * (i % 2)) + 8) % 8

    def z_send(p, to_stage, step):
        ref = wv.at[core, p % 4, g, f, :, w_cols(p)]
        return remote(ref, ref, zs.at[to_stage], zr.at[to_stage], at_z(step))

    def f_copy(i, from_f, lane, step):
        p = piece(i)
        ref = wv.at[core, p % 4, g, (from_f + 4) % 4, :, w_cols(p)]
        return remote(ref, ref, fs.at[i, lane], fr.at[i, lane], at_f(step))

    def s_copy(i, from_g, lane, step):
        p = piece(i)
        ref = wv.at[core, p % 4, (from_g + 4) % 4, :, :, w_cols(p)]
        return remote(ref, ref, ss.at[i, lane], sr.at[i, lane], at_g(step))

    def s_half(i, from_g, lane, step):
        p = piece(i)
        ref = wv.at[core, p % 4, (from_g + 4) % 4, pl.ds(2 * (lane - 2), 2), :, w_cols(p)]
        return remote(ref, ref, ss.at[i, lane], sr.at[i, lane], at_g(step))

    def d_copy(i, from_core):
        p = piece(i)
        ref = wv.at[from_core, p % 4, :, :, :, w_cols(p)]
        return remote(ref, ref, ds.at[i], dr.at[i], partner)

    def out_copy(i, from_core):
        p = piece(i)
        where = (from_core, p % 4, slice(None), slice(None), slice(None), w_cols(p))
        return pltpu.make_async_copy(wv.at[where], wb.at[where], lw.at[from_core, i])

    def weight_tick(t):
        @pl.when(t == 0)
        def _():
            z_send(z, 1, 1).start()
            z_send(z, 2, -1).start()

        @pl.when((t > 0) & (t < STAGES))
        def _():
            z_send(piece(t), t, 1).wait_recv()

            @pl.when((t <= 4) | ((t == 5) & (core == 0)) | ((t == 6) & (core == 1)))
            def _():
                z_send(piece(t), jnp.minimum(t + 2, 7), 2 * (t % 2) - 1).start()

        @pl.when(t < STAGES)
        def _():
            f_copy(t, f, 0, 1).start()
            f_copy(t, f, 1, -1).start()

        @pl.when((t >= 1) & (t < STAGES + 1))
        def _():
            i = t - 1
            f_copy(i, f - 1, 0, 1).wait_recv()
            f_copy(i, f + 1, 1, -1).wait_recv()
            sign = 1 - 2 * (i % 2)
            f_copy(i, f - sign, 2, sign).start()

        @pl.when((t >= 2) & (t < STAGES + 2))
        def _():
            i = t - 2
            f_copy(i, f + 2, 2, 1).wait_recv()
            s_copy(i, g, 0, 1).start()
            s_copy(i, g, 1, -1).start()

        @pl.when((t >= 3) & (t < STAGES + 3))
        def _():
            i = t - 3
            s_copy(i, g - 1, 0, 1).wait_recv()
            s_copy(i, g + 1, 1, -1).wait_recv()
            s_half(i, g - 1, 2, 1).start()
            s_half(i, g + 1, 3, -1).start()

        @pl.when((t >= 4) & (t < STAGES + 4))
        def _():
            i = t - 4
            s_half(i, g + 2, 2, 1).wait_recv()
            s_half(i, g + 2, 3, -1).wait_recv()
            d_copy(i, core).start()
            out_copy(i, core).start()

        @pl.when((t >= 5) & (t < STAGES + 5))
        def _():
            i = t - 5
            d_copy(i, 1 - core).wait_recv()
            out_copy(i, 1 - core).start()

    kv_begin(0)

    def tick(t, _):
        weight_tick(t)

        @pl.when(t < CHUNKS - 1)
        def _():
            kv_begin(t + 1)

        @pl.when((t >= 1) & (t < CHUNKS + 1))
        def _():
            kv_near(t - 1)
            kv_far(t - 1)

        @pl.when((t >= 2) & (t < CHUNKS + 2))
        def _():
            kv_last(t - 2)

        @pl.when((t >= 3) & (t < CHUNKS + 3))
        def _():
            kv_done(t - 3)
            attend(t - 3)

        return 0

    lax.fori_loop(0, TICKS + 1, tick, 0)

    def finish(i, _):
        sent(0, i)

        @pl.when(to_opposite)
        def _():
            sent(1, i)

        sent(2, i)

        @pl.when(jnp.logical_not(b_second))
        def _():
            sent(3, i)

        @pl.when(b_first)
        def _():
            sent(4, i)

        @pl.when(jnp.logical_or(b_first, jnp.logical_and(a_second, jnp.logical_not(last_of_four))))
        def _():
            sent(5, i)

        d_copy(i, core).wait_send()
        for lane in range(3):
            f_copy(i, f, lane, 1).wait_send()
        for lane in range(2):
            s_copy(i, g, lane, 1).wait_send()
            s_half(i, g, lane + 2, 1).wait_send()
        out_copy(i, 0).wait()
        out_copy(i, 1).wait()

        @pl.when(i > 0)
        def _():
            z_send(piece(i), i, 1).wait_send()

        return 0

    lax.fori_loop(0, STAGES, finish, 0)


def exchange(lengths, queries, keys, values, weight):
    anyspace = pl.BlockSpec(memory_space=pl.ANY)
    vmem = pl.BlockSpec(memory_space=pltpu.VMEM)
    dma = pltpu.SemaphoreType.DMA
    return pl.pallas_call(
        exchange_kernel,
        out_shape=(
            jax.ShapeDtypeStruct((ROWS, QUERY_HEADS * HEAD_SIZE), jnp.bfloat16),
            jax.ShapeDtypeStruct((2, 4, 4, 4, 16, D), jnp.bfloat16),
        ),
        in_specs=[vmem, anyspace, anyspace, anyspace, anyspace],
        out_specs=(vmem, anyspace),
        scratch_shapes=[
            pltpu.VMEM((ROWS, QUERY_HEADS * HEAD_SIZE), jnp.bfloat16),
            pltpu.VMEM((WINDOW + ROWS, 1024), jnp.bfloat16),
            pltpu.VMEM((WINDOW + ROWS, 1024), jnp.bfloat16),
            pltpu.VMEM((2, 4, 4, 4, 16, D), jnp.bfloat16),
            pltpu.VMEM((ROWS, 1), jnp.int32),
            dma((4,)), dma((2, 8)),
            dma((8,)), dma((8,)),
            dma((8, 3)), dma((8, 3)),
            dma((8, 4)), dma((8, 4)),
            dma((8,)), dma((8,)),
            dma((6, CHUNKS, 2)), dma((4, CHUNKS, 2)),
        ],
        compiler_params=pltpu.CompilerParams(
            collective_id=0, has_side_effects=True, vmem_limit_bytes=56 * 1024 * 1024
        ),
        name="exchange",
    )(lengths, queries, keys, values, weight)


def low_bound(lengths, offset):
    row = lax.broadcasted_iota(jnp.int32, (64, 64), 0)
    col = lax.broadcasted_iota(jnp.int32, (64, 64), 1)
    starts_col = jnp.sum(jnp.where(col < row, lengths, 0), axis=1, keepdims=True)
    starts = jnp.sum(jnp.where(row == col, starts_col, 0), axis=0, keepdims=True)
    i = lax.broadcasted_iota(jnp.int32, (ROWS, 1), 0)
    begins = jnp.max(jnp.where(starts <= i + offset, starts, 0), axis=1, keepdims=True)
    return jnp.maximum(begins - offset + WINDOW, i + 1)


TILE = 768
TILES = D // TILE


def project_kernel(a_ref, w_ref, res_ref, gain_ref, o_ref, acc, square):
    n = pl.program_id(0)
    slabs = []
    for x in range(4):
        for y in range(4):
            for zl in range(4):
                slabs.append(w_ref[0, zl, y, x])
                slabs.append(w_ref[1, zl, x, y])
    weight = jnp.concatenate(slabs, axis=0)
    part = jnp.dot(a_ref[...], weight, preferred_element_type=jnp.float32)
    acc[n] = part
    here = jnp.sum(part * part, axis=1, keepdims=True)

    @pl.when(n == 0)
    def _():
        square[...] = here

    @pl.when(n > 0)
    def _():
        square[...] += here

    @pl.when(n == TILES - 1)
    def _():
        level = lax.rsqrt(square[...] * (1.0 / D) + 1e-06)
        for m in range(TILES):
            columns = slice(TILE * m, TILE * m + TILE)
            normed = gain_ref[:, columns] * acc[m] * level
            o_ref[:, columns] = (res_ref[:, columns].astype(jnp.float32) + normed).astype(jnp.bfloat16)


def project(attended, wb, residual, gain):
    return pl.pallas_call(
        project_kernel,
        grid=(TILES,),
        out_shape=jax.ShapeDtypeStruct((ROWS, D), jnp.bfloat16),
        in_specs=[
            pl.BlockSpec((ROWS, QUERY_HEADS * HEAD_SIZE), lambda n: (0, 0)),
            pl.BlockSpec((2, 4, 4, 4, 16, TILE), lambda n: (0, 0, 0, 0, 0, n)),
            pl.BlockSpec((ROWS, D), lambda n: (0, 0)),
            pl.BlockSpec((1, D), lambda n: (0, 0)),
        ],
        out_specs=pl.BlockSpec((ROWS, D), lambda n: (0, 0)),
        scratch_shapes=[
            pltpu.VMEM((TILES, ROWS, TILE), jnp.float32),
            pltpu.VMEM((ROWS, 1), jnp.float32),
        ],
        compiler_params=pltpu.CompilerParams(vmem_limit_bytes=48 * 1024 * 1024),
        name="project",
    )(attended, wb, residual, gain)


def shards(queries, key_rotated_rows, values, out_weight, residual, norm_gain, doc_lengths):
    attended, wb = exchange(doc_lengths.reshape(1, 64), queries, key_rotated_rows, values, out_weight)
    return project(attended, wb, residual, norm_gain.reshape(1, D))


def solution(mesh):
    rows = P(("seq", "fsdp"), None)
    in_specs = (rows, rows, rows, P("seq", "fsdp"), rows, P(), P())
    return jax.shard_map(shards, mesh=mesh, in_specs=in_specs, out_specs=rows, check_vma=False)
```
